32 devices in a mesh: dp: 2 (over x), sp: 16 (over y, z, core).
Axes of the slice: x: 2, y: 2, z: 4, core: 2. Of those that a mesh axis runs over, the one named last changes fastest.
Arguments:
- q: bfloat16 [64, 56, 128], P('dp'), parts along dimension 0
- k: bfloat16 [64, 8192, 8, 128], P('dp', 'sp'), parts along dimension 0
- v: bfloat16 [64, 8192, 8, 128], P('dp', 'sp'), parts along dimension 0
Outputs:
- q: bfloat16 [64, 56, 128], P('dp'), parts along dimension 0
There are 2 independent parts. The reference program is written for one: setup_inputs(seed, part) draws one part's arguments, and reference() takes and returns one part's arrays. A program takes and returns all parts, laid end to end along the dimension named above; each array names one.
All inputs are finite; a program needn't handle non-finite values.
Results may differ from the reference program's by a relative error of at most 0.012.
Values are sent between devices in bfloat16 or wider.
A program may use at most 2 GiB of HBM per device.

```python
import jax
import jax.numpy as jnp

BATCH = 32
CACHE = 8192
HEADS = 56
KV_HEADS = 8
HEAD = 128


def setup_inputs(seed: int = 0, part: int = 0) -> dict:
    kq, kk, kv = (jax.random.fold_in(k, part) for k in jax.random.split(jax.random.key(seed), 3))
    return {
        "q": (3 * jax.random.normal(kq, (BATCH, HEADS, HEAD), jnp.float32)).astype(jnp.bfloat16),
        "k": jax.random.normal(kk, (BATCH, CACHE, KV_HEADS, HEAD), jnp.float32).astype(jnp.bfloat16),
        "v": jax.random.normal(kv, (BATCH, CACHE, KV_HEADS, HEAD), jnp.float32).astype(jnp.bfloat16),
    }


def einsum(form, a, b):
    return jnp.einsum(form, a.astype(jnp.float32), b.astype(jnp.float32))


def reference(q, k, v):
    grouped = q.reshape(BATCH, KV_HEADS, -1, HEAD)
    scores = einsum("bgsd,bugd->bgsu", grouped, k) * HEAD**-0.5
    weights = jax.nn.softmax(scores, -1).astype(jnp.bfloat16)
    return einsum("bgsu,bugd->bgsd", weights, v).astype(jnp.bfloat16).reshape(BATCH, HEADS, HEAD)
```

```python
import math

import jax
import jax.numpy as jnp
from jax import lax
from jax.experimental import pallas as pl
from jax.experimental.pallas import tpu as pltpu
from jax.sharding import PartitionSpec as P

MESH = pl.DeviceIdType.MESH
SLOTS = 6
LAG = 5
G = 8
W = 256


def kernel(q_ref, k_ref, v_ref, o_ref, kbuf, vbuf, qbuf, qq, bias, sbuf, hbuf, ksem, vsem, qsem,
           near_out, near_out_st, near_in, near_in_st, mine, mine_st, far_out, far_out_st, far_in, far_in_st, owned, owned_st, done,
           near_send, near_recv, far_send, far_recv, all_send, all_recv, done_sem):
    B, H, D = q_ref.shape
    S = H // G
    half = k_ref.shape[1] // 2
    NC = half // W
    T = H // 8
    pairs = B // 2
    c = D ** -0.5 * math.log2(math.e)
    me = lax.axis_index("sp")
    n = lax.axis_size("sp")
    chips = n // 2
    core = lax.rem(me, 2)
    chip = me // 2

    def seq(j, u):
        return 2 * j + core if u else 2 * j + 1 - core

    def owner(j):
        r = lax.rem(j, chips)
        x = lax.rem(3 + 2 * (r // 2), 5)
        z = x - 3 * (x // 4)
        z = z + core * (3 - 2 * z)
        return lax.rem(r + core, 2) * 4 + z

    def kcopy(j, u):
        s = lax.rem(2 * j + u, SLOTS)
        return pltpu.make_async_copy(k_ref.at[seq(j, u)], kbuf.at[s], ksem.at[s])

    def vcopy(j, u):
        s = lax.rem(2 * j + u, SLOTS)
        return pltpu.make_async_copy(v_ref.at[seq(j, u)], vbuf.at[s], vsem.at[s])

    def near(j):
        to = {"sp": me + 1 - 2 * core}
        return [
            pltpu.make_async_remote_copy(near_out.at[j], near_in.at[j], near_send.at[0, j], near_recv.at[0, j], device_id=to, device_id_type=MESH),
            pltpu.make_async_remote_copy(near_out_st.at[j], near_in_st.at[j], near_send.at[1, j], near_recv.at[1, j], device_id=to, device_id_type=MESH),
        ]

    def far(j, at, to):
        s = j // chips
        to = {"sp": 2 * to + core}
        return [
            pltpu.make_async_remote_copy(far_out.at[j], far_in.at[s, at], far_send.at[0, j], far_recv.at[0, s, at], device_id=to, device_id_type=MESH),
            pltpu.make_async_remote_copy(far_out_st.at[j], far_in_st.at[s, at], far_send.at[1, j], far_recv.at[1, s, at], device_id=to, device_id_type=MESH),
        ]

    def spread(j, i, b):
        return pltpu.make_async_remote_copy(done.at[j // chips], o_ref.at[b], all_send.at[j // chips, i], all_recv.at[b],
                                            device_id={"sp": lax.rem(me + i, n)}, device_id_type=MESH)

    def kept(j, b):
        return pltpu.make_async_copy(done.at[j // chips], o_ref.at[b], done_sem.at[j // chips])

    barrier = pltpu.get_barrier_semaphore()
    for i in range(1, n):
        pl.semaphore_signal(barrier, inc=1, device_id={"sp": lax.rem(me + i, n)}, device_id_type=MESH)
    qc = pltpu.make_async_copy(q_ref, qbuf, qsem)
    qc.start()
    held = SLOTS // 2
    for j in range(held + 1):
        for u in range(2):
            if j < held:
                kcopy(j, u).start()
            if j >= 1:
                vcopy(j - 1, u).start()
    row = lax.broadcasted_iota(jnp.int32, (H, W), 0)
    col = lax.broadcasted_iota(jnp.int32, (H, W), 1)
    bias[...] = jnp.where(row // S == lax.rem(col, G), jnp.inf, -jnp.inf)
    lane = lax.broadcasted_iota(jnp.int32, (8, 128), 1)
    qc.wait()

    def prep(b, _):
        x = qbuf[b].astype(jnp.float32)
        z = jnp.zeros_like(x)
        qq[b] = jnp.concatenate([jnp.concatenate([x, z], 1), jnp.concatenate([z, x], 1)], 0).astype(jnp.bfloat16)
        return 0
    lax.fori_loop(0, B, prep, 0)

    def side(buf, slot, i):
        return jnp.concatenate([buf[slot, i * W:(i + 1) * W], buf[slot, half + i * W:half + (i + 1) * W]], 1)

    def attend(jv, jk, us, outs):
        bb = bias[...]
        bb = jnp.concatenate([bb, bb], 0)
        if jv is not None:
            highs = {u: jnp.max(hbuf[u], 1, keepdims=True) for u in us}
        for u in us:
            high = total = acc = None
            if jv is not None:
                high2 = jnp.concatenate([highs[u], highs[u]], 0)
                vslot = lax.rem(2 * jv + u, SLOTS)
            if jk is not None:
                lhs = qq[seq(jk, u)]
                kslot = lax.rem(2 * jk + u, SLOTS)
            for i in range(NC):
                if jv is not None:
                    p = jnp.exp2((sbuf[u, i] - high2) * c)
                    h = p[:, :128] + p[:, 128:]
                    total = h if total is None else total + h
                    a = lax.dot_general(p.astype(jnp.bfloat16), side(vbuf, vslot, i), (((1,), (0,)), ((), ())), preferred_element_type=jnp.float32)
                    acc = a if acc is None else acc + a
                if jk is not None:
                    s = lax.dot_general(lhs, side(kbuf, kslot, i), (((1,), (1,)), ((), ())), preferred_element_type=jnp.float32)
                    s = jnp.minimum(s, bb)
                    sbuf[u, i] = s
                    h = jnp.maximum(s[:, :128], s[:, 128:])
                    h = jnp.maximum(h[:H], h[H:])
                    high = h if high is None else jnp.maximum(high, h)
            if jk is not None:
                hbuf[u] = high
            if jv is not None:
                total = jnp.sum(total[:H] + total[H:], 1, keepdims=True)
                outs(u, acc[:H, :D] + acc[H:, D:], stats(highs[u], total))

    def stats(high, total):
        st = jnp.zeros((8, 128), jnp.float32)
        for t in range(T):
            st = jnp.where(lane == t, high[8 * t:8 * t + 8], st)
            st = jnp.where(lane == 64 + t, total[8 * t:8 * t + 8], st)
        return st

    def scaled(acc, w):
        return [acc[8 * t:8 * t + 8] * w[:, t:t + 1] for t in range(T)]

    def merge(parts):
        high = parts[0]
        for st in parts[1:]:
            high = jnp.maximum(high, st)
        ws = [jnp.exp2((st - high) * c) for st in parts]
        total = None
        for st, w in zip(parts, ws):
            x = w * pltpu.roll(st, 64, 1)
            total = x if total is None else total + x
        return ws, high, total

    def outs(j):
        def f(u, acc, st):
            if u == 0:
                near_out[j] = acc.astype(jnp.bfloat16)
                near_out_st[j] = st
                for x in near(j):
                    x.start()
            else:
                mine[lax.rem(j, 2)] = acc
                mine_st[lax.rem(j, 2)] = st
        return f

    def join(j):
        for x in near(j):
            x.wait_recv()
        sa, sb = mine_st[lax.rem(j, 2)], near_in_st[j]
        (wa, wb), high, total = merge([sa, sb])
        st = jnp.where(lane < 64, high, pltpu.roll(total, 64, 1))
        xa = scaled(mine[lax.rem(j, 2)], wa)
        xb = scaled(near_in[j].astype(jnp.float32), wb)
        acc = jnp.concatenate([x + y for x, y in zip(xa, xb)], 0)
        to = owner(j)

        @pl.when(to == chip)
        def _():
            owned[j // chips] = acc
            owned_st[j // chips] = st

        @pl.when(to != chip)
        def _():
            far_out[j] = acc.astype(jnp.bfloat16)
            far_out_st[j] = st
            for x in far(j, chip, to):
                x.start()

    def finish(j):
        @pl.when(owner(j) == chip)
        def _():
            s = j // chips
            b = seq(j, 1)
            others = [lax.rem(chip + i, chips) for i in range(1, chips)]
            for x in others:
                for y in far(j, x, chip):
                    y.wait_recv()
            ws, _, total = merge([owned_st[s]] + [far_in_st[s, x] for x in others])
            inverse = 1.0 / total
            rows = scaled(owned[s], ws[0] * inverse)
            for x, w in zip(others, ws[1:]):
                rows = [y + z for y, z in zip(rows, scaled(far_in[s, x].astype(jnp.float32), w * inverse))]
            done[s] = jnp.concatenate(rows, 0).astype(jnp.bfloat16)
            for i in range(1, n):
                spread(j, i, b).start()
            kept(j, b).start()

    for u in range(2):
        kcopy(0, u).wait()
    attend(None, 0, (0, 1), None)
    for u in range(2):
        kcopy(held, u).start()
    pl.semaphore_wait(barrier, n - 1)

    def step(j, _):
        for u in range(2):
            vcopy(j, u).wait()
            kcopy(j + 1, u).wait()
        attend(j, j + 1, (0, 1), outs(j))
        for u in range(2):
            @pl.when(j + held < pairs)
            def _():
                vcopy(j + held, u).start()

            @pl.when(j + 1 + held < pairs)
            def _():
                kcopy(j + 1 + held, u).start()

        @pl.when(j >= 1)
        def _():
            join(j - 1)

        @pl.when(j >= LAG)
        def _():
            finish(j - LAG)
        return 0

    lax.fori_loop(0, pairs - 1, step, 0)
    last = pairs - 1
    for u in range(2):
        vcopy(last, u).wait()
        attend(last, None, (u,), outs(last))
    join(last - 1)
    join(last)
    lax.fori_loop(last - LAG, pairs, lambda j, _: (finish(j), 0)[1], 0)

    def drain(j, _):
        for x in near(j):
            x.wait_send()

        @pl.when(owner(j) != chip)
        def _():
            for x in far(j, chip, owner(j)):
                x.wait_send()

        @pl.when(owner(j) == chip)
        def _():
            b = seq(j, 1)
            for i in range(1, n):
                spread(j, i, b).wait_send()
            kept(j, b).wait()
        return 0
    lax.fori_loop(0, pairs, drain, 0)

    def arrive(j, _):
        spread(j, 1, seq(j, 0)).wait_recv()

        @pl.when(owner(j) != chip)
        def _():
            spread(j, 1, seq(j, 1)).wait_recv()
        return 0
    lax.fori_loop(0, pairs, arrive, 0)


def solution(mesh):
    n = mesh.shape["sp"]

    def step(q, k, v):
        B, L, _, D = k.shape
        H = q.shape[1]
        rows = L * G
        pairs = B // 2
        chips = n // 2
        own = pairs // chips
        f32, bf16, vmem, dma = jnp.float32, jnp.bfloat16, pltpu.VMEM, pltpu.SemaphoreType.DMA
        return pl.pallas_call(
            kernel,
            out_shape=jax.ShapeDtypeStruct(q.shape, q.dtype),
            in_specs=[pl.BlockSpec(memory_space=pl.ANY)] * 3,
            out_specs=pl.BlockSpec(memory_space=pl.ANY),
            scratch_shapes=[
                vmem((SLOTS, rows, D), bf16), vmem((SLOTS, rows, D), bf16), vmem((B, H, D), bf16), vmem((B, 2 * H, 2 * D), bf16),
                vmem((H, W), f32), vmem((2, rows // (2 * W), 2 * H, W), f32), vmem((2, H, 128), f32),
                dma((SLOTS,)), dma((SLOTS,)), dma,
                vmem((pairs, H, D), bf16), vmem((pairs, 8, 128), f32), vmem((pairs, H, D), bf16), vmem((pairs, 8, 128), f32),
                vmem((2, H, D), f32), vmem((2, 8, 128), f32),
                vmem((pairs, H, D), bf16), vmem((pairs, 8, 128), f32),
                vmem((own, chips, H, D), bf16), vmem((own, chips, 8, 128), f32),
                vmem((own, H, D), f32), vmem((own, 8, 128), f32), vmem((own, H, D), bf16),
                dma((2, pairs)), dma((2, pairs)), dma((2, pairs)), dma((2, own, chips)), dma((own, n)), dma((B,)), dma((own,)),
            ],
            compiler_params=pltpu.CompilerParams(vmem_limit_bytes=58 << 20, collective_id=0, has_side_effects=True),
            name="attend",
        )(q, k.reshape(B, rows, D), v.reshape(B, rows, D))

    return jax.shard_map(
        step,
        mesh=mesh,
        in_specs=(P("dp", None, None), P("dp", "sp", None, None), P("dp", "sp", None, None)),
        out_specs=P("dp", None, None),
        check_vma=False,
    )
```

```python
import functools
import math

import jax
import jax.numpy as jnp
from jax import lax
from jax.experimental import pallas as pl
from jax.experimental.pallas import tpu as pltpu
from jax.sharding import PartitionSpec as P

MESH = pl.DeviceIdType.MESH
SLOTS = 8
AHEAD = 3
LAG = 7
HAND = 6
G = 8
W = 256


def kernel(q_ref, k_ref, v_ref, o_ref, kbuf, vbuf, qbuf, qq, bias, sbuf, pbuf, hbuf, mbuf, tbuf, ksem, vsem, qsem,
           near_out, near_out_st, near_in, near_in_st, mine, mine_st, far_out, far_out_st, far_in, far_in_st, done,
           near_send, near_recv, far_send, far_recv, all_send, all_recv):
    B, H, D = q_ref.shape
    S = H // G
    half = k_ref.shape[1] // 2
    NC = half // W
    T = H // 8
    pairs = B // 2
    c = D ** -0.5 * math.log2(math.e)
    me = lax.axis_index("sp")
    n = lax.axis_size("sp")
    chips = n // 2
    core = me & 1
    chip = me >> 1

    def seq(j, u):
        return 2 * j + core if u else 2 * j + 1 - core

    def owner(j):
        low, high = (j >> 1) & 1, (j >> 2) & 1
        z = (2 * (1 ^ low) + (1 ^ low ^ high)) ^ (3 * core)
        return 4 * ((j ^ core) & 1) + z

    def slot(j, u):
        return (2 * j + u) & (SLOTS - 1)

    def kcopy(j, u):
        s = slot(j, u)
        return pltpu.make_async_copy(k_ref.at[seq(j, u)], kbuf.at[s], ksem.at[s])

    def vcopy(j, u):
        s = slot(j, u)
        return pltpu.make_async_copy(v_ref.at[seq(j, u)], vbuf.at[s], vsem.at[s])

    def near(j):
        to = {"sp": me + 1 - 2 * core}
        return [
            pltpu.make_async_remote_copy(near_out.at[j], near_in.at[j], near_send.at[0, j], near_recv.at[0, j], device_id=to, device_id_type=MESH),
            pltpu.make_async_remote_copy(near_out_st.at[j], near_in_st.at[j], near_send.at[1, j], near_recv.at[1, j], device_id=to, device_id_type=MESH),
        ]

    def far(j, at, to):
        s = j >> 3
        to = {"sp": 2 * to + core}
        return [
            pltpu.make_async_remote_copy(far_out.at[j], far_in.at[s, at], far_send.at[0, j], far_recv.at[0, s, at], device_id=to, device_id_type=MESH),
            pltpu.make_async_remote_copy(far_out_st.at[j], far_in_st.at[s, at], far_send.at[1, j], far_recv.at[1, s, at], device_id=to, device_id_type=MESH),
        ]

    def spread(j, b, slot, chip_, core_):
        i = 2 * chip_ + core_
        return pltpu.make_async_remote_copy(done.at[j >> 3], o_ref.at[b], all_send.at[slot, j], all_recv.at[b],
                                            device_id={"sp": i}, device_id_type=MESH)

    def spreads(j, b):
        y, z = chip >> 2, chip & 3
        to = [(((y + dy) & 1) * 4 + ((z + dz) & 3), core) for dy, dz in ((1, 2), (0, 2), (1, 1), (1, 3), (0, 1), (0, 3), (1, 0))]
        return [spread(j, b, i, *x) for i, x in enumerate(to + [(chip, 1 - core)])]

    def forward(b, j):
        return pltpu.make_async_remote_copy(o_ref.at[b], o_ref.at[b], all_send.at[0, j], all_recv.at[b],
                                            device_id={"sp": me + 1 - 2 * core}, device_id_type=MESH)

    barrier = pltpu.get_barrier_semaphore()
    for i in range(1, n):
        pl.semaphore_signal(barrier, inc=1, device_id={"sp": lax.rem(me + i, n)}, device_id_type=MESH)
    qc = pltpu.make_async_copy(q_ref, qbuf, qsem)
    qc.start()
    held = AHEAD

    def fetch(copy, j):
        for u in range(2):
            copy(j, u).start(priority=1)

    def await_(copy, j):
        for u in range(2):
            copy(j, u).wait()

    fetch(kcopy, 0)
    fetch(kcopy, 1)
    fetch(vcopy, 0)
    row = lax.broadcasted_iota(jnp.int32, (H, W), 0)
    col = lax.broadcasted_iota(jnp.int32, (H, W), 1)
    bias[...] = jnp.where(row // S == lax.rem(col, G), jnp.inf, -jnp.inf)
    lane = lax.broadcasted_iota(jnp.int32, (8, 128), 1)
    qc.wait()

    def prep(b, _):
        x = qbuf[b].astype(jnp.float32)
        z = jnp.zeros_like(x)
        qq[b] = jnp.concatenate([jnp.concatenate([x, z], 1), jnp.concatenate([z, x], 1)], 0).astype(jnp.bfloat16)
        return 0
    lax.fori_loop(0, B, prep, 0)

    def side(buf, slot, i):
        return jnp.concatenate([buf[slot, i * W:(i + 1) * W], buf[slot, half + i * W:half + (i + 1) * W]], 1)

    def attend(jv, je, jk, us, outs):
        if jv is not None:
            totals = {u: jnp.sum(tbuf[u], 1, keepdims=True) for u in us}
            for u in us:
                vslot = slot(jv, u)
                acc = None
                for i in range(NC):
                    a = lax.dot_general(pbuf[u, i], side(vbuf, vslot, i), (((1,), (0,)), ((), ())), preferred_element_type=jnp.float32)
                    acc = a if acc is None else acc + a
                outs(u, acc[:H, :D] + acc[H:, D:], stats(mbuf[u], totals[u]))
        if je is not None:
            for u in us:
                high = jnp.broadcast_to(jnp.max(hbuf[u], 1, keepdims=True), (H, 128))
                mbuf[u] = high
                high = jnp.concatenate([jnp.concatenate([high, high], 1)] * 2, 0)
                total = None
                for i in range(NC):
                    p = jnp.exp2((sbuf[u, i] - high) * c)
                    pbuf[u, i] = p.astype(jnp.bfloat16)
                    h = p[:, :128] + p[:, 128:]
                    h = h[:H] + h[H:]
                    total = h if total is None else total + h
                tbuf[u] = total
        if jk is not None:
            bb = bias[...]
            bb = jnp.concatenate([bb, bb], 0)
            for u in us:
                lhs = qq[seq(jk, u)]
                kslot = slot(jk, u)
                high = None
                for i in range(NC):
                    x = lax.dot_general(lhs, side(kbuf, kslot, i), (((1,), (1,)), ((), ())), preferred_element_type=jnp.float32)
                    x = jnp.minimum(x, bb)
                    sbuf[u, i] = x
                    h = jnp.maximum(x[:, :128], x[:, 128:])
                    h = jnp.maximum(h[:H], h[H:])
                    high = h if high is None else jnp.maximum(high, h)
                hbuf[u] = high

    def stats(high, total):
        st = jnp.zeros((8, 128), jnp.float32)
        for t in range(T):
            st = jnp.where(lane == t, high[8 * t:8 * t + 8], st)
            st = jnp.where(lane == 64 + t, total[8 * t:8 * t + 8], st)
        return st

    def scaled(acc, w):
        return [acc[8 * t:8 * t + 8] * w[:, t:t + 1] for t in range(T)]

    def merge(parts):
        high = parts[0]
        for st in parts[1:]:
            high = jnp.maximum(high, st)
        ws = [jnp.exp2((st - high) * c) for st in parts]
        total = None
        for st, w in zip(parts, ws):
            x = w * pltpu.roll(st, 64, 1)
            total = x if total is None else total + x
        return ws, high, total

    def outs(j):
        def f(u, acc, st):
            if u == 0:
                near_out[j] = acc.astype(jnp.bfloat16)
                near_out_st[j] = st
            else:
                mine[j] = acc
                mine_st[j] = st
        return f

    def join(j):
        (wa, wb), high, total = merge([mine_st[j], near_in_st[j]])
        st = jnp.where(lane < 64, high, pltpu.roll(total, 64, 1))
        xa = scaled(mine[j], wa)
        xb = scaled(near_in[j].astype(jnp.float32), wb)
        acc = jnp.concatenate([x + y for x, y in zip(xa, xb)], 0)
        mine[j] = acc
        mine_st[j] = st
        far_out[j] = acc.astype(jnp.bfloat16)
        far_out_st[j] = st

    def near_wait(j):
        for x in near(j):
            x.wait_recv()

    def near_start(j):
        for x in near(j):
            x.start()

    def far_start(j):
        to = owner(j)

        @pl.when(to != chip)
        def _():
            for x in far(j, chip, to):
                x.start()

    def finish(j):
        @pl.when(owner(j) == chip)
        def _():
            s = j >> 3
            b = seq(j, 1)
            others = [(chip + i) & (chips - 1) for i in range(1, chips)]
            for x in others:
                for y in far(j, x, chip):
                    y.wait_recv()
            ws, _, total = merge([mine_st[j]] + [far_in_st[s, x] for x in others])
            inverse = 1.0 / total
            rows = scaled(mine[j], ws[0] * inverse)
            for x, w in zip(others, ws[1:]):
                rows = [y + z for y, z in zip(rows, scaled(far_in[s, x].astype(jnp.float32), w * inverse))]
            done[s] = jnp.concatenate(rows, 0).astype(jnp.bfloat16)
            for x in spreads(j, b):
                x.start()
            o_ref[b] = done[s]

    def hand(j):
        @pl.when(owner(j) != chip)
        def _():
            b = seq(j, 1)
            forward(b, j).wait_recv()
            forward(b, j).start()

    both = (0, 1)
    await_(kcopy, 0)
    fetch(kcopy, 2)
    fetch(vcopy, 1)
    attend(None, None, 0, both, None)
    fetch(kcopy, 3)
    await_(kcopy, 1)
    attend(None, 0, 1, both, None)
    fetch(vcopy, 2)
    fetch(kcopy, 4)

    def step(joins, j, _):
        await_(vcopy, j)
        await_(kcopy, j + 2)
        if joins:
            near_wait(j - 2)
            join(j - 2)
        attend(j, j + 1, j + 2, both, outs(j))
        if not joins:
            @pl.when(j == 0)
            def _():
                pl.semaphore_wait(barrier, n - 1)
        near_start(j)
        if joins:
            far_start(j - 2)

        @pl.when(j + held < pairs)
        def _():
            fetch(vcopy, j + held)

        @pl.when(j + 2 + held < pairs)
        def _():
            fetch(kcopy, j + 2 + held)
        if joins:
            @pl.when(j >= LAG)
            def _():
                finish(j - LAG)

            @pl.when(j >= LAG + HAND)
            def _():
                hand(j - LAG - HAND)
        return 0

    last = pairs - 1
    lax.fori_loop(0, 2, functools.partial(step, False), 0)
    lax.fori_loop(2, last - 1, functools.partial(step, True), 0)
    await_(vcopy, last - 1)
    near_wait(last - 3)
    join(last - 3)
    attend(last - 1, last, None, both, outs(last - 1))
    near_start(last - 1)
    far_start(last - 3)
    near_wait(last - 2)
    join(last - 2)
    far_start(last - 2)
    vcopy(last, 0).wait()
    attend(last, None, None, (0,), outs(last))
    near_start(last)
    finish(last - 1 - LAG)
    near_wait(last - 1)
    join(last - 1)
    far_start(last - 1)
    vcopy(last, 1).wait()
    attend(last, None, None, (1,), outs(last))
    near_wait(last)
    join(last)
    far_start(last)
    lax.fori_loop(pairs - 1 - LAG, pairs, lambda j, _: (finish(j), 0)[1], 0)
    lax.fori_loop(last - 1 - LAG - HAND, pairs, lambda j, _: (hand(j), 0)[1], 0)

    def drain(j):
        for x in near(j):
            x.wait_send()

        @pl.when(owner(j) != chip)
        def _():
            for x in far(j, chip, owner(j)):
                x.wait_send()
            forward(seq(j, 1), j).wait_send()

        @pl.when(owner(j) == chip)
        def _():
            for x in spreads(j, seq(j, 1)):
                x.wait_send()
    for j in range(pairs):
        drain(j)

    def arrive(j):
        forward(seq(j, 0), j).wait_recv()
    for j in range(pairs):
        arrive(j)


def solution(mesh):
    n = mesh.shape["sp"]

    def step(q, k, v):
        B, L, _, D = k.shape
        H = q.shape[1]
        rows = L * G
        pairs = B // 2
        chips = n // 2
        own = pairs // chips
        f32, bf16, vmem, dma = jnp.float32, jnp.bfloat16, pltpu.VMEM, pltpu.SemaphoreType.DMA
        return pl.pallas_call(
            kernel,
            out_shape=pltpu.VMEM(q.shape, q.dtype),
            in_specs=[pl.BlockSpec(memory_space=pl.ANY)] * 3,
            out_specs=pl.BlockSpec(memory_space=pltpu.VMEM),
            scratch_shapes=[
                vmem((SLOTS, rows, D), bf16), vmem((SLOTS, rows, D), bf16), vmem((B, H, D), bf16), vmem((B, 2 * H, 2 * D), bf16),
                vmem((H, W), f32), vmem((2, rows // (2 * W), 2 * H, W), f32), vmem((2, rows // (2 * W), 2 * H, W), bf16),
                vmem((2, H, 128), f32), vmem((2, H, 128), f32), vmem((2, H, 128), f32),
                dma((SLOTS,)), dma((SLOTS,)), dma,
                vmem((pairs, H, D), bf16), vmem((pairs, 8, 128), f32), vmem((pairs, H, D), bf16), vmem((pairs, 8, 128), f32),
                vmem((pairs, H, D), f32), vmem((pairs, 8, 128), f32),
                vmem((pairs, H, D), bf16), vmem((pairs, 8, 128), f32),
                vmem((own, chips, H, D), bf16), vmem((own, chips, 8, 128), f32),
                vmem((own, H, D), bf16),
                dma((2, pairs)), dma((2, pairs)), dma((2, pairs)), dma((2, own, chips)), dma((chips, pairs)), dma((B,)),
            ],
            compiler_params=pltpu.CompilerParams(vmem_limit_bytes=58 << 20, collective_id=0, has_side_effects=True),
            name="attend",
        )(q, k.reshape(B, rows, D), v.reshape(B, rows, D))

    return jax.shard_map(
        step,
        mesh=mesh,
        in_specs=(P("dp", None, None), P("dp", "sp", None, None), P("dp", "sp", None, None)),
        out_specs=P("dp", None, None),
        check_vma=False,
    )
```

```python
import functools
import math

import jax
import jax.numpy as jnp
from jax import lax
from jax.experimental import pallas as pl
from jax.experimental.pallas import tpu as pltpu
from jax.sharding import PartitionSpec as P

MESH = pl.DeviceIdType.MESH
SLOTS = 8
AHEAD = 3
LAG = 7
HAND = 6
LATE = 1
G = 8
W = 256


def kernel(q_ref, k_ref, v_ref, o_ref, kbuf, vbuf, qbuf, qq, bias, sbuf, pbuf, hbuf, mbuf, tbuf, ksem, vsem, qsem,
           near_out, near_out_st, near_in, near_in_st, mine, mine_st, far_out, far_out_st, far_in, far_in_st, done,
           near_send, near_recv, far_send, far_recv, all_send, all_recv, late_send):
    B, H, D = q_ref.shape
    S = H // G
    half = k_ref.shape[1] // 2
    NC = half // W
    T = H // 8
    pairs = B // 2
    c = D ** -0.5 * math.log2(math.e)
    me = lax.axis_index("sp")
    n = lax.axis_size("sp")
    chips = n // 2
    core = me & 1
    chip = me >> 1

    def seq(j, u):
        return 2 * j + core if u else 2 * j + 1 - core

    def owner(j, core=core):
        low, high = (j >> 1) & 1, (j >> 2) & 1
        z = (2 * (1 ^ low) + (1 ^ low ^ high)) ^ (3 * core)
        return 4 * ((j ^ core) & 1) + z

    def slot(j, u):
        return (2 * j + u) & (SLOTS - 1)

    def kcopy(j, u):
        s = slot(j, u)
        return pltpu.make_async_copy(k_ref.at[seq(j, u)], kbuf.at[s], ksem.at[s])

    def vcopy(j, u):
        s = slot(j, u)
        return pltpu.make_async_copy(v_ref.at[seq(j, u)], vbuf.at[s], vsem.at[s])

    def near(j):
        to = {"sp": me + 1 - 2 * core}
        return [
            pltpu.make_async_remote_copy(near_out.at[j], near_in.at[j], near_send.at[0, j], near_recv.at[0, j], device_id=to, device_id_type=MESH),
            pltpu.make_async_remote_copy(near_out_st.at[j], near_in_st.at[j], near_send.at[1, j], near_recv.at[1, j], device_id=to, device_id_type=MESH),
        ]

    def far(j, at, to):
        s = j >> 3
        to = {"sp": 2 * to + core}
        return [
            pltpu.make_async_remote_copy(far_out.at[j], far_in.at[s, at], far_send.at[0, j], far_recv.at[0, s, at], device_id=to, device_id_type=MESH),
            pltpu.make_async_remote_copy(far_out_st.at[j], far_in_st.at[s, at], far_send.at[1, j], far_recv.at[1, s, at], device_id=to, device_id_type=MESH),
        ]

    first_late = pairs - LATE
    late_place = far_in.shape[0] - LATE

    def far_late(j, at, to):
        s = late_place + j - first_late
        to = {"sp": 2 * to + 1}
        return [
            pltpu.make_async_remote_copy(far_out.at[j], far_in.at[s, at], far_send.at[0, j], far_recv.at[0, s, at], device_id=to, device_id_type=MESH),
            pltpu.make_async_remote_copy(far_out_st.at[j], far_in_st.at[s, at], far_send.at[1, j], far_recv.at[1, s, at], device_id=to, device_id_type=MESH),
        ]

    def spreads_late(j):
        y, z = chip >> 2, chip & 3
        to = [4 * ((y + dy) & 1) + ((z + dz) & 3) for dy, dz in ((1, 2), (0, 2), (1, 1), (1, 3), (0, 1), (0, 3), (1, 0))]
        to = [2 * x + u for x in to for u in range(2)] + [2 * chip]
        x = j - first_late
        return [pltpu.make_async_remote_copy(done.at[late_place + x], o_ref.at[2 * j], late_send.at[x, i], all_recv.at[2 * j],
                                             device_id={"sp": d}, device_id_type=MESH) for i, d in enumerate(to)]

    def spread(j, b, slot, chip_, core_):
        i = 2 * chip_ + core_
        return pltpu.make_async_remote_copy(done.at[j >> 3], o_ref.at[b], all_send.at[slot, j], all_recv.at[b],
                                            device_id={"sp": i}, device_id_type=MESH)

    def spreads(j, b):
        y, z = chip >> 2, chip & 3
        to = [(((y + dy) & 1) * 4 + ((z + dz) & 3), core) for dy, dz in ((1, 2), (0, 2), (1, 1), (1, 3), (0, 1), (0, 3), (1, 0))]
        return [spread(j, b, i, *x) for i, x in enumerate(to + [(chip, 1 - core)])]

    def forward(b, j):
        return pltpu.make_async_remote_copy(o_ref.at[b], o_ref.at[b], all_send.at[0, j], all_recv.at[b],
                                            device_id={"sp": me + 1 - 2 * core}, device_id_type=MESH)

    barrier = pltpu.get_barrier_semaphore()
    for i in range(1, n):
        pl.semaphore_signal(barrier, inc=1, device_id={"sp": lax.rem(me + i, n)}, device_id_type=MESH)
    qc = pltpu.make_async_copy(q_ref, qbuf, qsem)
    qc.start()
    held = AHEAD

    def fetch(copy, j):
        for u in range(2):
            copy(j, u).start(priority=1)

    def await_(copy, j):
        for u in range(2):
            copy(j, u).wait()

    fetch(kcopy, 0)
    fetch(kcopy, 1)
    fetch(vcopy, 0)
    row = lax.broadcasted_iota(jnp.int32, (H, W), 0)
    col = lax.broadcasted_iota(jnp.int32, (H, W), 1)
    bias[...] = jnp.where(row // S == lax.rem(col, G), jnp.inf, -jnp.inf)
    lane = lax.broadcasted_iota(jnp.int32, (8, 128), 1)
    qc.wait()

    def prep(b, _):
        x = qbuf[b].astype(jnp.float32)
        z = jnp.zeros_like(x)
        qq[b] = jnp.concatenate([jnp.concatenate([x, z], 1), jnp.concatenate([z, x], 1)], 0).astype(jnp.bfloat16)
        return 0
    lax.fori_loop(0, B, prep, 0)

    def side(buf, slot, i):
        return jnp.concatenate([buf[slot, i * W:(i + 1) * W], buf[slot, half + i * W:half + (i + 1) * W]], 1)

    def attend(jv, je, jk, us, outs):
        if jv is not None:
            totals = {u: jnp.sum(tbuf[u], 1, keepdims=True) for u in us}
            for u in us:
                vslot = slot(jv, u)
                acc = None
                for i in range(NC):
                    a = lax.dot_general(pbuf[u, i], side(vbuf, vslot, i), (((1,), (0,)), ((), ())), preferred_element_type=jnp.float32)
                    acc = a if acc is None else acc + a
                outs(u, acc[:H, :D] + acc[H:, D:], stats(mbuf[u], totals[u]))
        if je is not None:
            for u in us:
                high = jnp.broadcast_to(jnp.max(hbuf[u], 1, keepdims=True), (H, 128))
                mbuf[u] = high
                high = jnp.concatenate([jnp.concatenate([high, high], 1)] * 2, 0)
                total = None
                for i in range(NC):
                    p = jnp.exp2((sbuf[u, i] - high) * c)
                    pbuf[u, i] = p.astype(jnp.bfloat16)
                    h = p[:, :128] + p[:, 128:]
                    h = h[:H] + h[H:]
                    total = h if total is None else total + h
                tbuf[u] = total
        if jk is not None:
            bb = bias[...]
            bb = jnp.concatenate([bb, bb], 0)
            for u in us:
                lhs = qq[seq(jk, u)]
                kslot = slot(jk, u)
                high = None
                for i in range(NC):
                    x = lax.dot_general(lhs, side(kbuf, kslot, i), (((1,), (1,)), ((), ())), preferred_element_type=jnp.float32)
                    x = jnp.minimum(x, bb)
                    sbuf[u, i] = x
                    h = jnp.maximum(x[:, :128], x[:, 128:])
                    h = jnp.maximum(h[:H], h[H:])
                    high = h if high is None else jnp.maximum(high, h)
                hbuf[u] = high

    def stats(high, total):
        st = jnp.zeros((8, 128), jnp.float32)
        for t in range(T):
            st = jnp.where(lane == t, high[8 * t:8 * t + 8], st)
            st = jnp.where(lane == 64 + t, total[8 * t:8 * t + 8], st)
        return st

    def scaled(acc, w):
        return [acc[8 * t:8 * t + 8] * w[:, t:t + 1] for t in range(T)]

    def merge(parts):
        high = parts[0]
        for st in parts[1:]:
            high = jnp.maximum(high, st)
        ws = [jnp.exp2((st - high) * c) for st in parts]
        total = None
        for st, w in zip(parts, ws):
            x = w * pltpu.roll(st, 64, 1)
            total = x if total is None else total + x
        return ws, high, total

    def outs(j):
        def f(u, acc, st):
            if u == 0:
                near_out[j] = acc.astype(jnp.bfloat16)
                near_out_st[j] = st
            else:
                mine[j] = acc
                mine_st[j] = st
        return f

    def join(j):
        (wa, wb), high, total = merge([mine_st[j], near_in_st[j]])
        st = jnp.where(lane < 64, high, pltpu.roll(total, 64, 1))
        xa = scaled(mine[j], wa)
        xb = scaled(near_in[j].astype(jnp.float32), wb)
        acc = jnp.concatenate([x + y for x, y in zip(xa, xb)], 0)
        mine[j] = acc
        mine_st[j] = st
        far_out[j] = acc.astype(jnp.bfloat16)
        far_out_st[j] = st

    def near_wait(j):
        for x in near(j):
            x.wait_recv()

    def near_start(j):
        for x in near(j):
            x.start()

    def far_start(j):
        to = owner(j)
        late = isinstance(j, int) and j >= first_late

        @pl.when((to != chip) & ((core == 1) | (not late)))
        def _():
            for x in far(j, chip, to):
                x.start()
        if late:
            @pl.when(core == 0)
            def _():
                for x in far_late(j, chip, owner(j, 0)):
                    x.start()

    def finish_late(j):
        @pl.when((core == 1) & (owner(j, 0) == chip))
        def _():
            s = late_place + j - first_late
            for x in range(chips):
                for y in far_late(j, x, chip):
                    y.wait_recv()
            ws, _, total = merge([far_in_st[s, x] for x in range(chips)])
            inverse = 1.0 / total
            rows = None
            for x, w in enumerate(ws):
                new = scaled(far_in[s, x].astype(jnp.float32), w * inverse)
                rows = new if rows is None else [y + z for y, z in zip(rows, new)]
            out = jnp.concatenate(rows, 0).astype(jnp.bfloat16)
            done[s] = out
            o_ref[2 * j] = out
            for x in spreads_late(j):
                x.start()

    def finish(j):
        @pl.when((owner(j) == chip) & ((core == 1) | (j < first_late)))
        def _():
            s = j >> 3
            b = seq(j, 1)
            others = [(chip + i) & (chips - 1) for i in range(1, chips)]
            for x in others:
                for y in far(j, x, chip):
                    y.wait_recv()
            ws, _, total = merge([mine_st[j]] + [far_in_st[s, x] for x in others])
            inverse = 1.0 / total
            rows = scaled(mine[j], ws[0] * inverse)
            for x, w in zip(others, ws[1:]):
                rows = [y + z for y, z in zip(rows, scaled(far_in[s, x].astype(jnp.float32), w * inverse))]
            done[s] = jnp.concatenate(rows, 0).astype(jnp.bfloat16)
            for x in spreads(j, b):
                x.start()
            o_ref[b] = done[s]

    def hand(j):
        @pl.when((owner(j) != chip) & ((core == 1) | (j < first_late)))
        def _():
            b = seq(j, 1)
            forward(b, j).wait_recv()
            forward(b, j).start()

    both = (0, 1)
    await_(kcopy, 0)
    fetch(kcopy, 2)
    fetch(vcopy, 1)
    attend(None, None, 0, both, None)
    fetch(kcopy, 3)
    await_(kcopy, 1)
    attend(None, 0, 1, both, None)
    fetch(vcopy, 2)
    fetch(kcopy, 4)

    def step(joins, j, _):
        await_(vcopy, j)
        await_(kcopy, j + 2)
        if joins:
            near_wait(j - 2)
            join(j - 2)
        attend(j, j + 1, j + 2, both, outs(j))
        if not joins:
            @pl.when(j == 0)
            def _():
                pl.semaphore_wait(barrier, n - 1)
        near_start(j)
        if joins:
            far_start(j - 2)

        @pl.when(j + held < pairs)
        def _():
            fetch(vcopy, j + held)

        @pl.when(j + 2 + held < pairs)
        def _():
            fetch(kcopy, j + 2 + held)
        if joins:
            @pl.when(j >= LAG)
            def _():
                finish(j - LAG)

            @pl.when(j >= LAG + HAND)
            def _():
                hand(j - LAG - HAND)
        return 0

    last = pairs - 1
    lax.fori_loop(0, 2, functools.partial(step, False), 0)
    lax.fori_loop(2, last - 1, functools.partial(step, True), 0)
    await_(vcopy, last - 1)
    near_wait(last - 3)
    join(last - 3)
    attend(last - 1, last, None, both, outs(last - 1))
    near_start(last - 1)
    far_start(last - 3)
    near_wait(last - 2)
    join(last - 2)
    far_start(last - 2)
    vcopy(last, 0).wait()
    attend(last, None, None, (0,), outs(last))
    near_start(last)
    finish(last - 1 - LAG)
    near_wait(last - 1)
    join(last - 1)
    far_start(last - 1)
    vcopy(last, 1).wait()
    attend(last, None, None, (1,), outs(last))
    near_wait(last)
    join(last)
    far_start(last)
    lax.fori_loop(pairs - 1 - LAG, pairs, lambda j, _: (finish(j), 0)[1], 0)
    lax.fori_loop(first_late, pairs, lambda j, _: (finish_late(j), 0)[1], 0)
    lax.fori_loop(last - 1 - LAG - HAND, pairs, lambda j, _: (hand(j), 0)[1], 0)

    for j in range(pairs):
        late = j >= first_late
        for x in near(j):
            x.wait_send()

        @pl.when((owner(j) != chip) & ((core == 1) | (not late)))
        def _():
            for x in far(j, chip, owner(j)):
                x.wait_send()
            forward(seq(j, 1), j).wait_send()

        @pl.when((owner(j) == chip) & ((core == 1) | (not late)))
        def _():
            for x in spreads(j, seq(j, 1)):
                x.wait_send()
        if late:
            @pl.when(core == 0)
            def _():
                for x in far_late(j, chip, owner(j, 0)):
                    x.wait_send()

            @pl.when((core == 1) & (owner(j, 0) == chip))
            def _():
                for x in spreads_late(j):
                    x.wait_send()
    for j in range(pairs):
        if j < first_late:
            forward(seq(j, 0), j).wait_recv()
        else:
            @pl.when((core == 0) | (owner(j, 0) != chip))
            def _():
                forward(2 * j, j).wait_recv()

            @pl.when(core == 0)
            def _():
                forward(2 * j + 1, j).wait_recv()


def solution(mesh):
    n = mesh.shape["sp"]

    def step(q, k, v):
        B, L, _, D = k.shape
        H = q.shape[1]
        rows = L * G
        pairs = B // 2
        chips = n // 2
        own = pairs // chips
        f32, bf16, vmem, dma = jnp.float32, jnp.bfloat16, pltpu.VMEM, pltpu.SemaphoreType.DMA
        return pl.pallas_call(
            kernel,
            out_shape=pltpu.VMEM(q.shape, q.dtype),
            in_specs=[pl.BlockSpec(memory_space=pl.ANY)] * 3,
            out_specs=pl.BlockSpec(memory_space=pltpu.VMEM),
            scratch_shapes=[
                vmem((SLOTS, rows, D), bf16), vmem((SLOTS, rows, D), bf16), vmem((B, H, D), bf16), vmem((B, 2 * H, 2 * D), bf16),
                vmem((H, W), f32), vmem((2, rows // (2 * W), 2 * H, W), f32), vmem((2, rows // (2 * W), 2 * H, W), bf16),
                vmem((2, H, 128), f32), vmem((2, H, 128), f32), vmem((2, H, 128), f32),
                dma((SLOTS,)), dma((SLOTS,)), dma,
                vmem((pairs, H, D), bf16), vmem((pairs, 8, 128), f32), vmem((pairs, H, D), bf16), vmem((pairs, 8, 128), f32),
                vmem((pairs, H, D), f32), vmem((pairs, 8, 128), f32),
                vmem((pairs, H, D), bf16), vmem((pairs, 8, 128), f32),
                vmem((own + LATE, chips, H, D), bf16), vmem((own + LATE, chips, 8, 128), f32),
                vmem((own + LATE, H, D), bf16),
                dma((2, pairs)), dma((2, pairs)), dma((2, pairs)), dma((2, own + LATE, chips)), dma((chips, pairs)), dma((B,)), dma((LATE, n)),
            ],
            compiler_params=pltpu.CompilerParams(vmem_limit_bytes=58 << 20, collective_id=0, has_side_effects=True),
            name="attend",
        )(q, k.reshape(B, rows, D), v.reshape(B, rows, D))

    return jax.shard_map(
        step,
        mesh=mesh,
        in_specs=(P("dp", None, None), P("dp", "sp", None, None), P("dp", "sp", None, None)),
        out_specs=P("dp", None, None),
        check_vma=False,
    )
```
